32 devices in a mesh: groups: 2 (over x), blk: 8 (over z, y), rep: 2 (over core).
Axes of the slice: x: 2, y: 2, z: 4, core: 2. Of those that a mesh axis runs over, the one named last changes fastest.
Arguments:
- tokens: bfloat16 [2048, 7168], P(('groups', 'blk', 'rep')), parts along dimension 0, may hold values from -6 to 6
- router_scores: float32 [2048, 8], P(('groups', 'blk', 'rep')), parts along dimension 0, may hold values from -6 to 6
- expert_ids: int32 [2048, 8], P(('groups', 'blk', 'rep')), parts along dimension 0, may hold values from 0 to 255, as said below
- gate_weight: bfloat16 [7168, 4096], P(None, ('blk', 'rep')), may hold values from -0.0625 to 0.0625
- up_weight: bfloat16 [7168, 4096], P(None, ('blk', 'rep')), may hold values from -0.0625 to 0.0625
- down_weight: bfloat16 [4096, 7168], P(('blk', 'rep')), may hold values from -0.125 to 0.125
Outputs:
- moe_out: bfloat16 [2048, 7168], P(('groups', 'blk', 'rep')), parts along dimension 0
The draws below stay inside these ranges and needn't reach their ends.
There are 2 independent parts, one for each index of `groups`. The reference program is written for one: setup_inputs(seed, part) draws one part's arguments, and reference() takes and returns one part's arrays. A program takes and returns all parts, laid end to end along the dimension named above; an argument that names none is the same for every part. Nothing has to cross between parts.
Inputs may be any that keep to these rules, and one draw needn't show every extreme that they name: `expert_ids`: each row names 8 different experts. In the rows of one device (aligned blocks of 64 rows) each expert below 2 is named by at most 2 rows, and in every draw one such expert is named by exactly 2 rows in every block.
All inputs are finite; a program needn't handle non-finite values.
Results may differ from the reference program's by a relative error of at most 0.0068.
Values may be sent and summed in bfloat16 or wider, within the bound.
No kernel may reach another device: no remote copies, remote signals or barrier semaphores. Data moves between devices by JAX's collectives and lax.ppermute only.
A program may use at most 128 MiB of HBM per device.

```python
import jax
import jax.numpy as jnp
from jax import lax

D = 7168
FF = 2048
EXPERTS = 256
TOP = 8
TOK_DEV = 64
CAP = 2
EXP_WIN = 2
TOKENS = 1024


def draw_block(block_key, hot_expert, expert_caps):
    key_count, key_rows, key_offset, key_order = jax.random.split(block_key, 4)
    counts = jax.random.randint(key_count, (EXP_WIN,), 0, expert_caps + 1)
    counts = jnp.where(jnp.arange(EXP_WIN) == hot_expert, CAP, counts)
    item_ends = jnp.cumsum(counts)
    total_items = item_ends[-1]
    item_index = jnp.arange(EXP_WIN * CAP)
    owners = jnp.sum((item_ends[None, :] <= item_index[:, None]).astype(jnp.int32), axis=1)
    is_valid = item_index < total_items
    row_order = jax.random.permutation(key_rows, TOK_DEV)
    item_row = jnp.where(is_valid, row_order[item_index % TOK_DEV], TOK_DEV)
    item_slot = item_index // TOK_DEV
    offsets = jax.random.randint(key_offset, (TOK_DEV, 1), 0, EXPERTS - EXP_WIN)
    outer_ids = EXP_WIN + (offsets + jnp.arange(TOP)[None, :]) % (EXPERTS - EXP_WIN)
    id_table = outer_ids.at[item_row, item_slot].set(owners, mode='drop')
    order_keys = jax.random.split(key_order, TOK_DEV)
    orders = jax.vmap(lambda one_key: jax.random.permutation(one_key, TOP))(order_keys)
    return jnp.take_along_axis(id_table, orders, axis=1).astype(jnp.int32)


def draw_expert_ids(key, part):
    num_blocks = TOKENS // TOK_DEV
    key_hot, key_caps, key_rest = jax.random.split(key, 3)
    hot_expert = jax.random.randint(key_hot, (), 0, EXP_WIN)
    expert_caps = jax.random.randint(key_caps, (EXP_WIN,), CAP // 2, CAP + 1)
    block_keys = jax.random.split(key_rest, num_blocks)
    id_blocks = jax.vmap(lambda one_key: draw_block(one_key, hot_expert, expert_caps))(block_keys)
    return id_blocks.reshape(TOKENS, TOP).astype(jnp.int32)


def steps_of(own_key, shape, cuts, low, high):
    def one(axis_at, shards_of):
        heights = jax.random.uniform(jax.random.fold_in(jax.random.fold_in(own_key, 6), axis_at), (shards_of,), jnp.float32, low / len(cuts), high / len(cuts))
        return jnp.repeat(jnp.exp(heights), shape[axis_at] // shards_of).reshape((-1,) + (1,) * (len(shape) - axis_at - 1))

    loudness = one(*cuts[0])
    for cut in cuts[1:]:
        loudness = loudness * one(*cut)
    return loudness


def noise(rng, dims, spread, most, pieces=(), kind=jnp.bfloat16):
    values = spread * jax.random.normal(rng, dims, jnp.float32)
    if pieces:
        values = values * steps_of(rng, dims, pieces, -0.22, 0.18)
    return jnp.clip(values, -most, most).astype(kind)


def setup_inputs(seed: int = 0, part: int = 0) -> dict:
    key_of = jax.random.split(jax.random.key(seed), 7)
    part_splits = jax.random.split(jax.random.fold_in(key_of[6], part), 7)
    return {
        "tokens": noise(part_splits[0], (TOKENS, D), 1.0, 6.0, ((0, 16),)),
        "router_scores": noise(part_splits[1], (TOKENS, TOP), 1.5, 6.0, ((0, 16),), jnp.float32),
        "expert_ids": draw_expert_ids(jax.random.fold_in(jax.random.fold_in(key_of[6], part), 71), part),
        "gate_weight": noise(key_of[3], (D, EXP_WIN * FF), D ** -0.5, 0.0625, ((1, 16),)),
        "up_weight": noise(key_of[4], (D, EXP_WIN * FF), D ** -0.5, 0.0625, ((1, 16),)),
        "down_weight": noise(key_of[5], (EXP_WIN * FF, D), FF ** -0.5, 0.125, ((0, 16),)),
    }


route_scale = 2.5


def reference(tokens, router_scores, expert_ids, gate_weight, up_weight, down_weight):
    sigmoid_scores = jax.nn.sigmoid(router_scores.astype(jnp.float32))
    gate_values = route_scale * sigmoid_scores / jnp.sum(sigmoid_scores, axis=1, keepdims=True)
    row_limit = CAP * (TOKENS // TOK_DEV)

    def one_expert(running, expert):
        member = expert_ids == expert
        weight_row = jnp.sum(jnp.where(member, gate_values, jnp.float32(0.0)), axis=1)
        is_named = jnp.any(member, axis=1)
        named_count = jnp.sum(is_named.astype(jnp.int32))
        positions = jnp.nonzero(is_named, size=row_limit, fill_value=0)[0].astype(jnp.int32)
        is_valid = jnp.arange(row_limit, dtype=jnp.int32) < named_count
        picked_rows = tokens[positions]
        first_unit = (expert * FF).astype(jnp.int32)
        w_gate = lax.dynamic_slice_in_dim(gate_weight, first_unit, FF, 1)
        w_up = lax.dynamic_slice_in_dim(up_weight, first_unit, FF, 1)
        w_down = lax.dynamic_slice_in_dim(down_weight, first_unit, FF, 0)
        gate_proj = jnp.dot(picked_rows, w_gate, preferred_element_type=jnp.float32)
        up_proj = jnp.dot(picked_rows, w_up, preferred_element_type=jnp.float32)
        hidden = (jax.nn.silu(gate_proj) * up_proj).astype(jnp.bfloat16)
        expert_out = jnp.dot(hidden, w_down, preferred_element_type=jnp.float32)
        row_weight = jnp.where(is_valid, weight_row[positions], jnp.float32(0.0))
        running = running.at[positions].add(row_weight[:, None] * expert_out)
        return running, None

    start_value = jnp.zeros((TOKENS, D), jnp.float32)
    combined, _ = lax.scan(one_expert, start_value, jnp.arange(EXP_WIN, dtype=jnp.int32))
    return combined.astype(jnp.bfloat16)
```

```python
import jax
import jax.numpy as jnp
from jax import lax
from jax.experimental import pallas as pl
from jax.experimental.pallas import tpu as pltpu
from jax.sharding import PartitionSpec as P

FF = 2048
CAP = 2


route_scale = 2.5


def ffn_kernel(mine_ref, other_ref, gate_ref, up_ref, down_ref, keep_ref, send_ref):
    half = mine_ref.shape[0]
    rows = jnp.concatenate([mine_ref[...], other_ref[...]], axis=0)
    gate_proj = jnp.dot(rows, gate_ref[...], preferred_element_type=jnp.float32)
    up_proj = jnp.dot(rows, up_ref[...], preferred_element_type=jnp.float32)
    hidden = (gate_proj / (1.0 + jnp.exp(-gate_proj)) * up_proj).astype(jnp.bfloat16)
    out = jnp.dot(hidden, down_ref[...], preferred_element_type=jnp.float32)
    keep_ref[...] = out[:half]
    send_ref[...] = out[half:].astype(jnp.bfloat16)


def expert_rows(mine, other, w_gate, w_up, w_down):
    rows, width = mine.shape
    return pl.pallas_call(
        ffn_kernel,
        out_shape=(
            jax.ShapeDtypeStruct((rows, width), jnp.float32),
            jax.ShapeDtypeStruct((rows, width), jnp.bfloat16),
        ),
        in_specs=[pl.BlockSpec(memory_space=pltpu.VMEM)] * 5,
        out_specs=[pl.BlockSpec(memory_space=pltpu.VMEM)] * 2,
        compiler_params=pltpu.CompilerParams(vmem_limit_bytes=40 * 1024 * 1024),
    )(mine, other, w_gate, w_up, w_down)


def shards(tokens, router_scores, expert_ids, gate_weight, up_weight, down_weight):
    blk_count = lax.axis_size("blk")
    rep_count = lax.axis_size("rep")
    model_width = tokens.shape[1]
    slice_units = gate_weight.shape[1]
    window_size = blk_count * rep_count * slice_units // FF
    group_size = blk_count // window_size
    swap = [(0, 1), (1, 0)]
    sigmoid_scores = jax.nn.sigmoid(router_scores)
    gate_values = route_scale * sigmoid_scores / jnp.sum(sigmoid_scores, axis=1, keepdims=True)
    expert_range = jnp.arange(window_size, dtype=jnp.int32)
    member = expert_ids[:, :, None] == expert_range[None, None, :]
    is_hit = jnp.any(member, axis=1)
    token_weight = jnp.sum(jnp.where(member, gate_values[:, :, None], jnp.float32(0.0)), axis=1)
    slot_rank = jnp.cumsum(is_hit.astype(jnp.int32), axis=0) - 1
    slot_range = jnp.arange(CAP, dtype=jnp.int32)
    placed = (slot_rank.T[:, None, :] == slot_range[None, :, None]) & is_hit.T[:, None, :]
    packed = jnp.einsum(
        "ect,td->ecd", placed.astype(jnp.bfloat16), tokens, preferred_element_type=jnp.float32
    ).astype(jnp.bfloat16)
    outgoing = jnp.repeat(packed, group_size, axis=0)
    arrived = lax.all_to_all(outgoing, "blk", split_axis=0, concat_axis=0, tiled=True)
    mine = arrived.reshape(-1, model_width)
    other = lax.ppermute(mine, "rep", swap)
    keep, send = expert_rows(mine, other, gate_weight, up_weight, down_weight)
    taken = lax.ppermute(send, "rep", swap)
    own_partial = (keep + taken.astype(jnp.float32)).astype(jnp.bfloat16)
    returned = lax.all_to_all(
        own_partial.reshape(blk_count, CAP, model_width), "blk", split_axis=0, concat_axis=0, tiled=True
    )
    per_expert = jnp.sum(
        returned.reshape(window_size, group_size, CAP, model_width).astype(jnp.float32), axis=1
    )
    weighted = jnp.where(placed, token_weight.T[:, None, :], jnp.float32(0.0))
    combined = jnp.einsum("ect,ecd->td", weighted, per_expert, precision=lax.Precision.HIGHEST)
    return combined.astype(jnp.bfloat16)


def solution(mesh):
    placed = (
        P(("groups", "blk", "rep"), None),
        P(("groups", "blk", "rep"), None),
        P(("groups", "blk", "rep"), None),
        P(None, ("blk", "rep")),
        P(None, ("blk", "rep")),
        P(("blk", "rep"), None),
    )
    return jax.shard_map(
        shards,
        mesh=mesh,
        in_specs=placed,
        out_specs=P(("groups", "blk", "rep"), None),
        check_vma=False,
    )
```

```python
from functools import partial

import jax
import jax.numpy as jnp
from jax import lax
from jax.experimental import pallas as pl
from jax.experimental.pallas import tpu as pltpu
from jax.sharding import PartitionSpec as P

FF = 2048
CAP = 2


route_scale = 2.5
LANES = 128
PREFETCH_COST = 10**9
VMEM = pl.BlockSpec(memory_space=pltpu.VMEM)
HBM = pl.BlockSpec(memory_space=pltpu.HBM)


def slots_of(ids, rows, window_size, group_size):
    top, count = ids.shape
    index = lax.broadcasted_iota(jnp.int32, (rows, count), 0)
    own_expert = lax.axis_index("blk") // group_size
    order = jnp.where(index < window_size * CAP, own_expert ^ (index // CAP), -1)
    members = [ids[slot : slot + 1] == order for slot in range(top)]
    hit = jnp.zeros((rows, count), jnp.float32)
    for member in members:
        hit = jnp.where(member, 1.0, hit)
    from_index = lax.broadcasted_iota(jnp.int32, (count, count), 0)
    to_index = lax.broadcasted_iota(jnp.int32, (count, count), 1)
    upper = jnp.where(from_index <= to_index, 1.0, 0.0).astype(jnp.bfloat16)
    rank = jnp.dot(hit.astype(jnp.bfloat16), upper, preferred_element_type=jnp.float32)
    placed = jnp.where(rank == (index % CAP + 1).astype(jnp.float32), hit, 0.0)
    return members, placed


def pack_kernel(window_size, group_size, ids_ref, tokens_ref, *refs):
    *packet_refs, ids_near, tokens_near, sems = refs
    ids_copy = pltpu.make_async_copy(ids_ref, ids_near, sems.at[0])
    tokens_copy = pltpu.make_async_copy(tokens_ref, tokens_near, sems.at[1])
    ids_copy.start()
    tokens_copy.start()
    rows = -(-window_size * CAP // 16) * 16
    ids_copy.wait()
    _, placed = slots_of(ids_near[...], rows, window_size, group_size)
    tokens_copy.wait()
    packed = jnp.dot(placed.astype(jnp.bfloat16), tokens_near[...], preferred_element_type=jnp.float32)
    for index, ref in enumerate(packet_refs):
        ref[...] = packed[index * CAP : (index + 1) * CAP].astype(jnp.bfloat16)


def weigh_kernel(window_size, group_size, scores_ref, ids_ref, weight_ref):
    sigmoid_scores = 1.0 / (1.0 + jnp.exp(-scores_ref[...]))
    gate_values = route_scale * sigmoid_scores / jnp.sum(sigmoid_scores, axis=0, keepdims=True)
    members, placed = slots_of(ids_ref[...], LANES, window_size, group_size)
    weight = jnp.zeros(placed.shape, jnp.float32)
    for slot, member in enumerate(members):
        weight = jnp.where(member, gate_values[slot : slot + 1], weight)
    weight_ref[...] = (placed * weight).T


def merge_kernel(*refs):
    out_ref = refs[-1]
    pieces = [ref[...].astype(jnp.float32) for ref in refs[:-1]]
    out_ref[...] = jnp.concatenate(pieces, axis=0).astype(jnp.bfloat16)


def merge(pieces, cost=0):
    rows = sum(piece.shape[0] for piece in pieces)
    return pl.pallas_call(
        merge_kernel,
        out_shape=jax.ShapeDtypeStruct((rows, pieces[0].shape[1]), jnp.bfloat16),
        in_specs=[VMEM] * len(pieces),
        out_specs=VMEM,
        cost_estimate=pl.CostEstimate(flops=cost, bytes_accessed=cost, transcendentals=0) if cost else None,
        compiler_params=pltpu.CompilerParams(vmem_limit_bytes=12 * 1024 * 1024),
    )(*pieces)


def fetch_kernel(source_ref, near_ref, sem):
    copy = pltpu.make_async_copy(source_ref, near_ref, sem)
    copy.start()
    copy.wait()


def fetch(array):
    return pl.pallas_call(
        fetch_kernel,
        out_shape=pltpu.VMEM(array.shape, array.dtype),
        in_specs=[HBM],
        out_specs=VMEM,
        scratch_shapes=[pltpu.SemaphoreType.DMA],
        compiler_params=pltpu.CompilerParams(vmem_limit_bytes=1024 * 1024),
    )(array)


def ffn_kernel(mine_ref, other_ref, gate_ref, up_ref, down_ref, keep_ref, send_ref):
    half = mine_ref.shape[0]
    blocks, block_rows, _ = keep_ref.shape
    rows = jnp.concatenate([mine_ref[...], other_ref[...]], axis=0)
    gate_proj = jnp.dot(rows, gate_ref[...], preferred_element_type=jnp.float32)
    up_proj = jnp.dot(rows, up_ref[...], preferred_element_type=jnp.float32)
    hidden = (gate_proj / (1.0 + jnp.exp(-gate_proj)) * up_proj).astype(jnp.bfloat16)
    out = jnp.dot(hidden, down_ref[...], preferred_element_type=jnp.float32)
    for block in range(blocks):
        first = block * block_rows
        keep_ref[block] = out[first : first + block_rows]
        send_ref[block] = out[half + first : half + first + block_rows].astype(jnp.bfloat16)


def expert_rows(mine, other, w_gate, w_up, w_down, blocks):
    rows, width = mine.shape
    shape = (blocks, rows // blocks, width)
    return pl.pallas_call(
        ffn_kernel,
        out_shape=(
            jax.ShapeDtypeStruct(shape, jnp.float32),
            jax.ShapeDtypeStruct(shape, jnp.bfloat16),
        ),
        in_specs=[VMEM] * 5,
        out_specs=(VMEM, VMEM),
        compiler_params=pltpu.CompilerParams(vmem_limit_bytes=28 * 1024 * 1024),
    )(mine, other, w_gate, w_up, w_down)


def combine_kernel(weight_ref, *refs):
    *part_refs, out_ref, stage_ref, sems = refs
    chunks = sems.shape[0]
    step = stage_ref.shape[1] // chunks
    weight = weight_ref[...]
    columns = [weight[:, column : column + 1] for column in range(len(part_refs) * CAP)]
    copies = []
    for chunk in range(chunks):
        span = pl.ds(chunk * step, step)
        total = jnp.zeros((stage_ref.shape[0], step), jnp.float32)
        for index, ref in enumerate(part_refs):
            part = ref[:, span].astype(jnp.float32)
            for slot in range(CAP):
                total = total + columns[index * CAP + slot] * part[slot : slot + 1]
        stage_ref[:, span] = total.astype(jnp.bfloat16)
        copies.append(
            pltpu.make_async_copy(stage_ref.at[:, span], out_ref.at[:, span], sems.at[chunk])
        )
        copies[-1].start()
    for copy in copies:
        copy.wait()


def combine(weight, parts, count):
    width = parts[0].shape[1]
    chunks = 7 if width % (7 * LANES) == 0 else 1
    return pl.pallas_call(
        combine_kernel,
        out_shape=jax.ShapeDtypeStruct((count, width), jnp.bfloat16),
        in_specs=[VMEM] * (len(parts) + 1),
        out_specs=HBM,
        scratch_shapes=[pltpu.VMEM((count, width), jnp.bfloat16), pltpu.SemaphoreType.DMA((chunks,))],
        compiler_params=pltpu.CompilerParams(vmem_limit_bytes=16 * 1024 * 1024),
    )(weight, *parts)


def shards(tokens, router_scores, expert_ids, gate_weight, up_weight, down_weight):
    blk_count = lax.axis_size("blk")
    rep_count = lax.axis_size("rep")
    count, model_width = tokens.shape
    slice_units = gate_weight.shape[1]
    window_size = blk_count * rep_count * slice_units // FF
    group_size = blk_count // window_size
    swap = [(0, 1), (1, 0)]

    def across(value, mask):
        return lax.ppermute(value, "blk", [(s, s ^ mask) for s in range(blk_count)])

    packets = pl.pallas_call(
        partial(pack_kernel, window_size, group_size),
        out_shape=[pltpu.VMEM((CAP, model_width), jnp.bfloat16)] * window_size,
        in_specs=[HBM] * 2,
        out_specs=[VMEM] * window_size,
        scratch_shapes=[
            pltpu.VMEM(expert_ids.shape[::-1], expert_ids.dtype),
            pltpu.VMEM(tokens.shape, tokens.dtype),
            pltpu.SemaphoreType.DMA((2,)),
        ],
        compiler_params=pltpu.CompilerParams(vmem_limit_bytes=66_500_000),
    )(expert_ids.T, tokens)
    far = []
    for k in range(1, window_size):
        far.append(across(packets[k], k * group_size))
    weight = pl.pallas_call(
        partial(weigh_kernel, window_size, group_size),
        out_shape=pltpu.VMEM((count, LANES), jnp.float32),
        in_specs=[VMEM] * 2,
        out_specs=VMEM,
        cost_estimate=pl.CostEstimate(flops=PREFETCH_COST, bytes_accessed=PREFETCH_COST, transcendentals=0),
        compiler_params=pltpu.CompilerParams(vmem_limit_bytes=2 * 1024 * 1024),
    )(router_scores.T, expert_ids.T)
    rows = merge([packets[0]] + far, cost=PREFETCH_COST)
    near = []
    for k in range(1, group_size):
        near.append(across(rows, k))
    down_near = fetch(down_weight)
    mine = merge([rows] + near)
    other = lax.ppermute(mine, "rep", swap)
    keep, send = expert_rows(mine, other, gate_weight, up_weight, down_near, group_size)
    taken = lax.ppermute(send, "rep", swap)
    total = keep + taken.astype(jnp.float32)
    leaving = total.astype(jnp.bfloat16)
    back = [across(leaving[k], k) for k in range(1, group_size)]
    block = total[0]
    for value in back:
        block = block + value.astype(jnp.float32)
    home = block[CAP:].astype(jnp.bfloat16)
    parts = [block] + [
        across(home[(k - 1) * CAP : k * CAP], k * group_size) for k in range(1, window_size)
    ]
    return combine(weight, parts, count)


def solution(mesh):
    placed = (
        P(("groups", "blk", "rep"), None),
        P(("groups", "blk", "rep"), None),
        P(("groups", "blk", "rep"), None),
        P(None, ("blk", "rep")),
        P(None, ("blk", "rep")),
        P(("blk", "rep"), None),
    )
    return jax.shard_map(
        shards,
        mesh=mesh,
        in_specs=placed,
        out_specs=P(("groups", "blk", "rep"), None),
        check_vma=False,
    )
```
